32 devices in a mesh: rep: 16 (over z, y, x), shard: 2 (over core).
Axes of the slice: x: 2, y: 2, z: 4, core: 2. Of those that a mesh axis runs over, the one named last changes fastest.
Arguments:
- outer_params: float32 [4, 131072], P('shard'), may hold values from -6 to 6
- replica_delta: float32 [16, 4, 131072], P('rep', 'shard'), may hold values from -20 to 20
- momentum: float32 [4, 131072], P('shard', 'rep'), may hold values from -20 to 20
- tensor_of_block: int32 [4], P('shard'), may hold values from 0 to 1, as said below
Outputs:
- new_params: float32 [4, 131072], P('shard')
- new_momentum: float32 [4, 131072], P('shard', 'rep')
The draws below stay inside these ranges and needn't reach their ends.
Inputs may be any that keep to these rules, and one draw needn't show every extreme that they name: `tensor_of_block`: every tensor owns exactly 2 blocks.
All inputs are finite; a program needn't handle non-finite values.
Results may differ from the reference program's by a relative error of at most 0.00028.
Values sent between devices are 32-bit elements; how exact they have to be, the bound alone decides.
No kernel may reach another device: no remote copies, remote signals or barrier semaphores. Data moves between devices by JAX's collectives and lax.ppermute only.
A program may use at most 64 MiB of HBM per device.

```python
import math
import jax
import jax.numpy as jnp
from jax import lax

BLOCK_ROWS = 128
BLOCK_COLS = 1024
NS_STEPS = 8
REPLICAS = 16
BLOCKS = 4
GROUPS = 2


def common_parts(key):
    base = jax.random.fold_in(key, 11)
    log_scale = jax.random.uniform(jax.random.fold_in(base, 1), (BLOCKS, 1), jnp.float32, math.log(0.5), math.log(2.0))
    shared = jnp.clip(jax.random.normal(jax.random.fold_in(base, 2), (BLOCKS, BLOCK_ROWS * BLOCK_COLS), jnp.float32), -5.0, 5.0)
    align = jax.random.uniform(jax.random.fold_in(base, 3), (BLOCKS, 1), jnp.float32, -1.0, 1.0)
    return (jnp.exp(log_scale), shared, align)


def draw_momentum(key, part):
    scale, shared, align = common_parts(key)
    noise = jnp.clip(jax.random.normal(jax.random.fold_in(key, 21), shared.shape, jnp.float32), -5.0, 5.0)
    values = 0.7 * scale * (align * shared + noise)
    return values.astype(jnp.float32)


def draw_replica_delta(key, part):
    scale, shared, align = common_parts(key)
    noise = jnp.clip(jax.random.normal(jax.random.fold_in(key, 31), (REPLICAS, BLOCKS, BLOCK_ROWS * BLOCK_COLS), jnp.float32), -5.0, 5.0)
    values = scale[None] * (shared[None] + noise)
    return values.astype(jnp.float32)


def draw_tensor_of_block(key, part):
    order = jax.random.permutation(jax.random.fold_in(key, 41), BLOCKS)
    return (order % GROUPS).astype(jnp.int32)


def block_levels(stream_key, shape, shards, least, high):
    def one(position, shards_of):
        steps = jax.random.uniform(jax.random.fold_in(jax.random.fold_in(stream_key, 6), position), (shards_of,), jnp.float32, least / len(shards), high / len(shards))
        return jnp.repeat(jnp.exp(steps), shape[position] // shards_of).reshape((-1,) + (1,) * (len(shape) - position - 1))

    factor_of = one(*shards[0])
    for cut in shards[1:]:
        factor_of = factor_of * one(*cut)
    return factor_of


def gaussian(key, extent, scale, reach, split=(), held_as=jnp.bfloat16):
    drawn = jax.random.normal(key, extent, jnp.float32) * scale
    if len(split) > 0:
        drawn = block_levels(key, extent, split, -0.22, 0.18) * drawn
    return jnp.clip(drawn, min=-reach, max=reach).astype(held_as)


def setup_inputs(seed: int = 0) -> dict:
    seeds = jax.random.split(jax.random.key(seed), 5)
    return {
        "outer_params": gaussian(seeds[0], (BLOCKS, BLOCK_ROWS * BLOCK_COLS), 1.0, 6.0, ((0, 2),), jnp.float32),
        "replica_delta": draw_replica_delta(jax.random.fold_in(seeds[4], 71), 0),
        "momentum": draw_momentum(jax.random.fold_in(seeds[4], 71), 0),
        "tensor_of_block": draw_tensor_of_block(jax.random.fold_in(seeds[4], 71), 0),
    }


outer_rate = 0.7
decay_rate = 0.9

def orthogonalize(direction):
    blocks = direction.reshape(direction.shape[0], BLOCK_ROWS, BLOCK_COLS)
    blocks = blocks / jnp.sqrt(lax.optimization_barrier(jnp.sum(blocks * blocks, axis=(1, 2), keepdims=True)) + 1.0)
    for step in range(NS_STEPS):
        square = jnp.einsum('bij,bkj->bik', blocks, blocks, precision=lax.Precision.HIGHEST)
        blocks = 1.5 * blocks - 0.5 * jnp.einsum('bik,bkj->bij', square, blocks, precision=lax.Precision.HIGHEST)
    return blocks.reshape(direction.shape[0], BLOCK_ROWS * BLOCK_COLS)

def reference(outer_params, replica_delta, momentum, tensor_of_block):
    mean_delta = lax.optimization_barrier(jnp.sum(replica_delta, axis=0)) / REPLICAS
    new_momentum = decay_rate * momentum + mean_delta
    direction = mean_delta + decay_rate * new_momentum
    update = orthogonalize(direction)
    member = (tensor_of_block[:, None] == jnp.arange(GROUPS, dtype=jnp.int32)[None, :]).astype(jnp.float32)
    per_block = jnp.stack([lax.optimization_barrier(jnp.sum(outer_params * outer_params, axis=1)), lax.optimization_barrier(jnp.sum(update * update, axis=1))], axis=1)
    tensor_sums = lax.optimization_barrier(jnp.sum(member[:, :, None] * per_block[:, None, :], axis=0))
    group_rate = outer_rate * jnp.sqrt(jnp.maximum(tensor_sums[:, 0], 1.0) / jnp.maximum(tensor_sums[:, 1], 1.0))
    block_rate = lax.optimization_barrier(jnp.sum(member * group_rate[None, :], axis=1))
    new_params = outer_params - block_rate[:, None] * update
    return (new_params, new_momentum)
```

```python
import jax
import jax.numpy as jnp
from jax import lax
from jax.experimental import pallas as pl
from jax.experimental.pallas import tpu as pltpu
from jax.sharding import PartitionSpec as P

BLOCK_ROWS = 128
BLOCK_COLS = 1024
NS_STEPS = 8
LANES = 128
CHUNKS = BLOCK_COLS // LANES


outer_rate = 0.7
decay_rate = 0.9

VMEM = pl.BlockSpec(memory_space=pltpu.VMEM)
SMEM = pl.BlockSpec(memory_space=pltpu.SMEM)


def interleave(a):
    blocks, n = a.shape
    return a.reshape(blocks, n // LANES, LANES).transpose(1, 0, 2).reshape(-1, LANES)


def deinterleave(a, blocks):
    rows = a.shape[0]
    return a.reshape(rows // blocks, blocks, LANES).transpose(1, 0, 2).reshape(blocks, -1)


def exchange(a, bit):
    size = lax.axis_size("rep")
    return lax.ppermute(a, "rep", [(i, i ^ (1 << bit)) for i in range(size)])


def shape(*dims):
    return jax.ShapeDtypeStruct(dims, jnp.float32)


def first_split(rank, x, replicas, firsts):
    n = x.shape[0] // replicas
    pieces = len(firsts)
    cut = n // pieces
    half = replicas // 2

    def body(rank_ref, x_ref, *outs):
        rank = rank_ref[0]
        for p, bit in enumerate(firsts):
            for side in (1, 0):
                picked = [m for m in range(replicas) if (m >> bit) & 1 == side]
                for at, m in enumerate(picked):
                    start = pl.multiple_of((rank ^ m) * n + p * cut, 8)
                    outs[2 * p + 1 - side][at * cut : (at + 1) * cut, :] = x_ref[
                        pl.ds(start, cut), :
                    ]

    outs = pl.pallas_call(
        body,
        out_shape=[shape(half * cut, LANES)] * (2 * pieces),
        in_specs=[SMEM, VMEM],
        out_specs=[VMEM] * (2 * pieces),
    )(rank, x)
    return [(outs[2 * p], outs[2 * p + 1]) for p in range(pieces)]


def reduce_stages(pairs, orders):
    bits = len(orders[0])
    alive = [sorted((b for b in range(bits) if b != o[0]), reverse=True) for o in orders]
    pairs = [list(pair) for pair in pairs]
    for stage in range(bits):
        got = [exchange(send, order[stage]) for (send, _), order in zip(pairs, orders)]
        if stage == bits - 1:
            return [(keep, recv) for (_, keep), recv in zip(pairs, got)]
        for p, order in enumerate(orders):
            keep = pairs[p][1]
            left = alive[p]
            rows = keep.shape[0] >> len(left)
            view = (2,) * len(left) + (rows, LANES)
            axis = left.index(order[stage + 1])
            keep, recv = keep.reshape(view), got[p].reshape(view)
            halves = [
                lax.index_in_dim(keep, side, axis, False) + lax.index_in_dim(recv, side, axis, False)
                for side in (1, 0)
            ]
            pairs[p] = [h.reshape(-1, LANES) for h in halves]
            left.pop(axis)


def nesterov(addends, momentum, replicas, blocks):
    n = momentum.shape[0]
    own_rows = n // (blocks * CHUNKS)
    cut = n // len(addends)

    def body(*refs):
        ins, mom_ref, new_ref = refs[: 2 * len(addends)], refs[2 * len(addends)], refs[2 * len(addends) + 1]
        dirs, scratch = refs[2 * len(addends) + 2 : -1], refs[-1]
        for p in range(len(addends)):
            rows = slice(p * cut, (p + 1) * cut)
            mean = (ins[2 * p][...] + ins[2 * p + 1][...]) / replicas
            new = decay_rate * mom_ref[rows, :] + mean
            new_ref[rows, :] = new
            scratch[rows, :] = mean + decay_rate * new
        for b in range(blocks):
            for c in range(CHUNKS):
                dirs[b][c * own_rows : (c + 1) * own_rows, :] = scratch[
                    pl.ds(c * blocks + b, own_rows, stride=CHUNKS * blocks), :
                ]

    outs = pl.pallas_call(
        body,
        out_shape=[shape(n, LANES)] + [shape(CHUNKS * own_rows, LANES)] * blocks,
        in_specs=[VMEM] * (2 * len(addends) + 1),
        out_specs=[VMEM] * (blocks + 1),
        scratch_shapes=[pltpu.VMEM((n, LANES), jnp.float32)],
    )(*[a for pair in addends for a in pair], momentum)
    return outs[0], outs[1:]


def gather_stages(own, orders):
    bits = len(orders[0])
    pieces = [a.reshape((1,) + a.shape) for a in own]
    done = [[] for _ in own]
    for stage in range(bits):
        got = [exchange(a, order[stage]) for a, order in zip(pieces, orders)]
        for p, order in enumerate(orders):
            pieces[p] = jnp.concatenate([pieces[p], got[p]], axis=0)
            done[p].insert(0, order[stage])
    owners = []
    for p in range(len(own)):
        owners.append(
            [
                sum(((i >> (bits - 1 - k)) & 1) << bit for k, bit in enumerate(done[p]))
                for i in range(1 << bits)
            ]
        )
    return pieces, owners


def split(a):
    hi = a.astype(jnp.bfloat16)
    return hi, (a - hi.astype(jnp.float32)).astype(jnp.bfloat16)


def dot(a, b, dims):
    return lax.dot_general(a, b, (dims, ((), ())), preferred_element_type=jnp.float32)


NN = ((1,), (0,))
NT = ((1,), (1,))


def dot3(a, b, dims=NN):
    (ah, al), (bh, bl) = a, b
    return dot(ah, bh, dims) + (dot(ah, bl, dims) + dot(al, bh, dims))


def newton_schulz(tiles):
    blocks = len(tiles)
    groups = tiles[0].shape[0]
    size = groups * 8

    def body(*refs):
        ins, outs, sums = refs[:blocks], refs[blocks : 2 * blocks], refs[2 * blocks]
        row = lax.broadcasted_iota(jnp.int32, (size, size), 0)
        col = lax.broadcasted_iota(jnp.int32, (size, size), 1)
        eye = (row == col).astype(jnp.float32)
        xs, squares, factors, scales = [], [], [], []
        for b in range(blocks):
            chunks = [split(ins[b][:, c].reshape(size, LANES)) for c in range(CHUNKS)]
            hi = jnp.concatenate([h for h, _ in chunks], axis=1)
            lo = jnp.concatenate([l for _, l in chunks], axis=1)
            gram = dot3((hi, lo), (hi, lo), NT)
            total = jnp.sum(jnp.sum(gram * eye, axis=1, keepdims=True), axis=0, keepdims=True) + 1.0
            squares.append(gram / total)
            scales.append(lax.rsqrt(total))
            factors.append(None)
            xs.append((hi, lo))
        for step in range(NS_STEPS):
            for b in range(blocks):
                factor = 1.5 * eye - 0.5 * squares[b]
                fs = split(factor)
                if step == 0:
                    factors[b] = factor
                else:
                    factors[b] = dot3(fs, split(factors[b]))
                if step < NS_STEPS - 1:
                    squares[b] = dot3(split(dot3(fs, split(squares[b]))), fs)
        for b in range(blocks):
            fs = split(factors[b] * scales[b])
            update = dot3(fs, xs[b])
            sums[b] = jnp.sum(update * update)
            for c in range(CHUNKS):
                outs[b][:, c] = update[:, c * LANES : (c + 1) * LANES].reshape(groups, 8, LANES)

    outs = pl.pallas_call(
        body,
        out_shape=[shape(*tiles[0].shape)] * blocks + [shape(blocks)],
        in_specs=[VMEM] * blocks,
        out_specs=[VMEM] * blocks + [SMEM],
    )(*tiles)
    return outs[:blocks], outs[blocks]


def apply_update(rank, rates, params, updates, owners):
    blocks = len(updates)
    stride = CHUNKS * blocks

    def body(rank_ref, rate_ref, params_ref, *refs):
        ins, out_ref = refs[:blocks], refs[blocks]
        rank = rank_ref[0]
        for b in range(blocks):
            rate = rate_ref[b]
            for i, m in enumerate(owners[b]):
                base = (rank ^ m) * (8 * stride)
                for c in range(CHUNKS):
                    rows = pl.ds(base + (c * blocks + b), 8, stride=stride)
                    out_ref[rows, :] = params_ref[rows, :] - rate * ins[b][i, c]

    return pl.pallas_call(
        body,
        out_shape=shape(*params.shape),
        in_specs=[SMEM, SMEM, VMEM] + [VMEM] * blocks,
        out_specs=VMEM,
    )(rank, rates, params, *updates)


def apply_update_plain(rank, rates, params, updates, owners, own_rows):
    blocks = len(updates)
    replicas = len(owners[0])
    fold = 8 // own_rows
    rows = []
    for b in range(blocks):
        u = updates[b].reshape(replicas // fold, CHUNKS, fold, own_rows, LANES)
        u = u.transpose(0, 2, 3, 1, 4).reshape(replicas, own_rows * CHUNKS * LANES)
        where = [0] * replicas
        for i, m in enumerate(owners[b]):
            where[m] = i
        order = jnp.array(where, jnp.int32)[jnp.arange(replicas, dtype=jnp.int32) ^ rank[0]]
        rows.append(jnp.take(u, order, axis=0).reshape(-1))
    return params - rates[:, None] * jnp.stack(rows)


def group_sums(member, params_sum, update_sum):
    per_block = jnp.stack([params_sum, update_sum], axis=1)
    return jnp.sum(member[:, :, None] * per_block[:, None, :], axis=0)


def block_rates(tensor_sums, member):
    group_rate = outer_rate * jnp.sqrt(
        jnp.maximum(tensor_sums[:, 0], 1.0) / jnp.maximum(tensor_sums[:, 1], 1.0)
    )
    return jnp.sum(member * group_rate[None, :], axis=1)


def shards(outer_params, replica_delta, momentum, tensor_of_block):
    replicas = lax.axis_size("rep")
    bits = replicas.bit_length() - 1
    blocks = outer_params.shape[0]
    own_rows = BLOCK_ROWS // replicas
    all_blocks = blocks * lax.axis_size("shard")
    tensors = max(all_blocks // 4, 2)
    member = (tensor_of_block[:, None] == jnp.arange(tensors, dtype=jnp.int32)[None, :]).astype(
        jnp.float32
    )
    rank = lax.axis_index("rep").astype(jnp.int32)[None]
    orders = [list(range(bits)), [1, 0] + list(range(2, bits))]
    pairs = first_split(rank, interleave(replica_delta[0]), replicas, [o[0] for o in orders])
    addends = reduce_stages(pairs, orders)
    new_momentum, own = nesterov(addends, interleave(momentum), replicas, blocks)
    pieces, owners = gather_stages(own, [orders[b % 2][::-1] for b in range(blocks)])
    if own_rows == 8:
        tiles = [a.reshape(replicas, CHUNKS, 8, LANES) for a in pieces]
    else:
        fold = 8 // own_rows
        tiles = [
            a.reshape(replicas // fold, fold, CHUNKS, own_rows, LANES)
            .transpose(0, 2, 1, 3, 4)
            .reshape(replicas // fold, CHUNKS, 8, LANES)
            for a in pieces
        ]
    updates, update_sum = newton_schulz(tiles)
    params_sum = jnp.sum(outer_params * outer_params, axis=1)
    tensor_sums = lax.psum(group_sums(member, params_sum, update_sum), "shard")
    rates = block_rates(tensor_sums, member)
    if own_rows == 8:
        new_params = apply_update(rank, rates, interleave(outer_params), updates, owners)
        new_params = deinterleave(new_params, blocks)
    else:
        new_params = apply_update_plain(rank, rates, outer_params, updates, owners, own_rows)
    return (new_params, deinterleave(new_momentum, blocks))


def solution(mesh):
    return jax.shard_map(
        shards,
        mesh=mesh,
        in_specs=(P("shard", None), P("rep", "shard", None), P("shard", "rep"), P("shard")),
        out_specs=(P("shard", None), P("shard", "rep")),
        check_vma=False,
    )
```

```python
import jax
import jax.numpy as jnp
from jax import lax
from jax.experimental import pallas as pl
from jax.experimental.pallas import tpu as pltpu
from jax.sharding import PartitionSpec as P

BLOCK_ROWS = 128
BLOCK_COLS = 1024
NS_STEPS = 8
LANES = 128
CHUNKS = BLOCK_COLS // LANES


outer_rate = 0.7
decay_rate = 0.9

VMEM = pl.BlockSpec(memory_space=pltpu.VMEM)
SMEM = pl.BlockSpec(memory_space=pltpu.SMEM)


def interleave(a):
    blocks, n = a.shape
    return a.reshape(blocks, n // LANES, LANES).transpose(1, 0, 2).reshape(-1, LANES)


def deinterleave(a, blocks):
    rows = a.shape[0]
    return a.reshape(rows // blocks, blocks, LANES).transpose(1, 0, 2).reshape(blocks, -1)


def in_vmem(a):
    return pltpu.with_memory_space_constraint(a, pltpu.VMEM)


def exchange(a, bit, axis="rep"):
    size = lax.axis_size(axis)
    return lax.ppermute(a, axis, [(i, i ^ (1 << bit)) for i in range(size)])


def shape(*dims):
    return jax.ShapeDtypeStruct(dims, jnp.float32)


def kept(*dims):
    return pltpu.VMEM(dims, jnp.float32)


def first_split(rank, x, replicas, firsts):
    n = x.shape[0] // replicas
    pieces = len(firsts)
    cut = n // pieces
    half = replicas // 2

    def body(rank_ref, x_ref, *outs):
        rank = rank_ref[0]
        for p, bit in enumerate(firsts):
            for side in (1, 0):
                picked = [m for m in range(replicas) if (m >> bit) & 1 == side]
                for at, m in enumerate(picked):
                    start = pl.multiple_of((rank ^ m) * n + p * cut, 8)
                    outs[2 * p + 1 - side][at * cut : (at + 1) * cut, :] = x_ref[
                        pl.ds(start, cut), :
                    ]

    outs = pl.pallas_call(
        body,
        out_shape=[kept(half * cut, LANES)] * (2 * pieces),
        in_specs=[SMEM, VMEM],
        out_specs=[VMEM] * (2 * pieces),
    )(rank, x)
    return [(outs[2 * p], outs[2 * p + 1]) for p in range(pieces)]


def reduce_stages(pairs, orders):
    bits = len(orders[0])
    alive = [sorted((b for b in range(bits) if b != o[0]), reverse=True) for o in orders]
    pairs = [list(pair) for pair in pairs]
    for stage in range(bits):
        got = [exchange(send, order[stage]) for (send, _), order in zip(pairs, orders)]
        if stage == bits - 1:
            return [(keep, recv) for (_, keep), recv in zip(pairs, got)]
        for p, order in enumerate(orders):
            keep = pairs[p][1]
            left = alive[p]
            rows = keep.shape[0] >> len(left)
            view = (2,) * len(left) + (rows, LANES)
            axis = left.index(order[stage + 1])
            keep, recv = keep.reshape(view), got[p].reshape(view)
            halves = [
                lax.index_in_dim(keep, side, axis, False) + lax.index_in_dim(recv, side, axis, False)
                for side in (1, 0)
            ]
            pairs[p] = [h.reshape(-1, LANES) for h in halves]
            left.pop(axis)


def nesterov(addends, momentum, replicas, blocks):
    n = momentum.shape[0]
    own_rows = n // (blocks * CHUNKS)
    cut = n // len(addends)

    def body(*refs):
        ins, mom_ref, new_ref = refs[: 2 * len(addends)], refs[2 * len(addends)], refs[2 * len(addends) + 1]
        dirs, scratch = refs[2 * len(addends) + 2 : -1], refs[-1]
        for p in range(len(addends)):
            rows = slice(p * cut, (p + 1) * cut)
            mean = (ins[2 * p][...] + ins[2 * p + 1][...]) / replicas
            new = decay_rate * mom_ref[rows, :] + mean
            new_ref[rows, :] = new
            scratch[rows, :] = mean + decay_rate * new
        for b in range(blocks):
            for c in range(CHUNKS):
                dirs[b][c * own_rows : (c + 1) * own_rows, :] = scratch[
                    pl.ds(c * blocks + b, own_rows, stride=CHUNKS * blocks), :
                ]

    outs = pl.pallas_call(
        body,
        out_shape=[shape(n, LANES)] + [kept(CHUNKS * own_rows, LANES)] * blocks,
        in_specs=[VMEM] * (2 * len(addends) + 1),
        out_specs=[VMEM] * (blocks + 1),
        scratch_shapes=[pltpu.VMEM((n, LANES), jnp.float32)],
    )(*[in_vmem(a) for pair in addends for a in pair], momentum)
    return outs[0], outs[1:]


def gather_stages(own, orders):
    bits = len(orders[0])
    pieces = [a.reshape((1,) + a.shape) for a in own]
    done = [[] for _ in own]
    for stage in range(bits):
        got = [exchange(a, order[stage]) for a, order in zip(pieces, orders)]
        for p, order in enumerate(orders):
            if stage == bits - 1:
                pieces[p] = [pieces[p], got[p]]
            else:
                pieces[p] = jnp.concatenate([pieces[p], got[p]], axis=0)
            done[p].insert(0, order[stage])
    owners = []
    for p in range(len(own)):
        owners.append(
            [
                sum(((i >> (bits - 1 - k)) & 1) << bit for k, bit in enumerate(done[p]))
                for i in range(1 << bits)
            ]
        )
    return pieces, owners


def split(a):
    hi = a.astype(jnp.bfloat16)
    return hi, (a - hi.astype(jnp.float32)).astype(jnp.bfloat16)


def dot(a, b, dims):
    return lax.dot_general(a, b, (dims, ((), ())), preferred_element_type=jnp.float32)


NN = ((1,), (0,))
NT = ((1,), (1,))


def dot3(a, b, dims=NN):
    (ah, al), (bh, bl) = a, b
    return dot(ah, bh, dims) + (dot(ah, bl, dims) + dot(al, bh, dims))


def newton_schulz(tiles, tensor_of_block, params_sum, tensors):
    blocks = len(tiles)
    parts = len(tiles[0])
    groups = sum(t.shape[0] for t in tiles[0])
    size = groups * 8

    def body(*refs):
        tob_ref, params_ref = refs[:2]
        ins, out, sums = refs[2:-2], refs[-2], refs[-1]
        tensor = lax.broadcasted_iota(jnp.int32, sums.shape, 0)
        kind = lax.broadcasted_iota(jnp.int32, sums.shape, 1)
        both = jnp.zeros(sums.shape, jnp.float32)
        row = lax.broadcasted_iota(jnp.int32, (size, size), 0)
        col = lax.broadcasted_iota(jnp.int32, (size, size), 1)
        eye = (row == col).astype(jnp.float32)
        xs, squares, factors, scales = [], [], [], []
        for b in range(blocks):
            own = ins[b * parts : (b + 1) * parts]
            chunks = [
                split(jnp.concatenate([a[:, c].reshape(-1, LANES) for a in own], axis=0))
                for c in range(CHUNKS)
            ]
            hi = jnp.concatenate([h for h, _ in chunks], axis=1)
            lo = jnp.concatenate([l for _, l in chunks], axis=1)
            gram = dot3((hi, lo), (hi, lo), NT)
            total = jnp.sum(jnp.sum(gram * eye, axis=1, keepdims=True), axis=0, keepdims=True) + 1.0
            squares.append(gram / total)
            scales.append(lax.rsqrt(total))
            factors.append(None)
            xs.append((hi, lo))
        for step in range(NS_STEPS):
            for b in range(blocks):
                factor = 1.5 * eye - 0.5 * squares[b]
                fs = split(factor)
                if step == 0:
                    factors[b] = factor
                else:
                    factors[b] = dot3(fs, split(factors[b]))
                if step < NS_STEPS - 1:
                    squares[b] = dot3(split(dot3(fs, split(squares[b]))), fs)
        for b in range(blocks):
            fs = split(factors[b] * scales[b])
            update = dot3(fs, xs[b])
            square = jnp.sum(jnp.sum(update * update, axis=0, keepdims=True), axis=1, keepdims=True)
            value = jnp.where(kind == 0, params_ref[b], jnp.where(kind == 1, square, 0.0))
            both = both + jnp.where(tensor == tob_ref[b], value, 0.0)
            for c in range(CHUNKS):
                out[b, :, c] = update[:, c * LANES : (c + 1) * LANES].reshape(groups, 8, LANES)
        sums[...] = both

    return pl.pallas_call(
        body,
        out_shape=[kept(blocks, groups, CHUNKS, 8, LANES), kept(-(-tensors // 8) * 8, LANES)],
        in_specs=[SMEM, SMEM] + [VMEM] * (blocks * parts),
        out_specs=[VMEM, VMEM],
    )(tensor_of_block, params_sum, *[in_vmem(t) for own in tiles for t in own])


def apply_update(rank, tensor_of_block, tensor_sums, params, updates, owners):
    blocks = updates.shape[0]
    stride = CHUNKS * blocks

    def body(rank_ref, tob_ref, sums_ref, params_ref, update_ref, out_ref):
        rank = rank_ref[0]
        sums = sums_ref[...]
        group_rate = outer_rate * jnp.sqrt(
            jnp.maximum(sums[:, 0:1], 1.0) / jnp.maximum(sums[:, 1:2], 1.0)
        )
        group_rate = jnp.broadcast_to(group_rate, sums.shape)
        tensor = lax.broadcasted_iota(jnp.int32, sums.shape, 0)
        for b in range(blocks):
            rate = jnp.where(tensor == tob_ref[b], group_rate, 0.0)
            rate = jnp.broadcast_to(jnp.sum(rate, axis=0, keepdims=True), (8, LANES))
            for i, m in enumerate(owners[b]):
                base = (rank ^ m) * (8 * stride)
                for c in range(CHUNKS):
                    rows = pl.ds(base + (c * blocks + b), 8, stride=stride)
                    out_ref[rows, :] = params_ref[rows, :] - rate * update_ref[b, i, c]

    return pl.pallas_call(
        body,
        out_shape=shape(*params.shape),
        in_specs=[SMEM, SMEM] + [VMEM] * 3,
        out_specs=VMEM,
    )(rank, tensor_of_block, in_vmem(tensor_sums), in_vmem(params), in_vmem(updates))


def apply_update_plain(rank, rates, params, updates, owners, own_rows):
    blocks = updates.shape[0]
    replicas = len(owners[0])
    fold = 8 // own_rows
    rows = []
    for b in range(blocks):
        u = updates[b].reshape(replicas // fold, CHUNKS, fold, own_rows, LANES)
        u = u.transpose(0, 2, 3, 1, 4).reshape(replicas, own_rows * CHUNKS * LANES)
        where = [0] * replicas
        for i, m in enumerate(owners[b]):
            where[m] = i
        order = jnp.array(where, jnp.int32)[jnp.arange(replicas, dtype=jnp.int32) ^ rank[0]]
        rows.append(jnp.take(u, order, axis=0).reshape(-1))
    return params - rates[:, None] * jnp.stack(rows)


def block_rates(tensor_sums, member):
    group_rate = outer_rate * jnp.sqrt(
        jnp.maximum(tensor_sums[:, 0], 1.0) / jnp.maximum(tensor_sums[:, 1], 1.0)
    )
    return jnp.sum(member * group_rate[None, :], axis=1)


def shards(outer_params, replica_delta, momentum, tensor_of_block):
    replicas = lax.axis_size("rep")
    bits = replicas.bit_length() - 1
    blocks = outer_params.shape[0]
    own_rows = BLOCK_ROWS // replicas
    all_blocks = blocks * lax.axis_size("shard")
    tensors = max(all_blocks // 4, 2)
    member = (tensor_of_block[:, None] == jnp.arange(tensors, dtype=jnp.int32)[None, :]).astype(
        jnp.float32
    )
    rank = lax.axis_index("rep").astype(jnp.int32)[None]
    orders = [list(range(bits)), [1, 0] + list(range(2, bits))]
    pairs = first_split(rank, interleave(replica_delta[0]), replicas, [o[0] for o in orders])
    addends = reduce_stages(pairs, orders)
    new_momentum, own = nesterov(addends, interleave(momentum), replicas, blocks)
    pieces, owners = gather_stages(own, [orders[b % 2][::-1] for b in range(blocks)])
    if own_rows == 8:
        tiles = [[a.reshape(-1, CHUNKS, 8, LANES) for a in halves] for halves in pieces]
    else:
        fold = 8 // own_rows
        tiles = [
            [
                jnp.concatenate(halves, axis=0)
                .reshape(replicas // fold, fold, CHUNKS, own_rows, LANES)
                .transpose(0, 2, 1, 3, 4)
                .reshape(replicas // fold, CHUNKS, 8, LANES)
            ]
            for halves in pieces
        ]
    params_sum = jnp.sum(outer_params * outer_params, axis=1)
    updates, sums = newton_schulz(tiles, tensor_of_block, params_sum, tensors)
    tensor_sums = sums
    for bit in range(lax.axis_size("shard").bit_length() - 1):
        tensor_sums = tensor_sums + exchange(tensor_sums, bit, "shard")
    if own_rows == 8:
        new_params = apply_update(
            rank, tensor_of_block, tensor_sums, interleave(outer_params), updates, owners
        )
        new_params = deinterleave(new_params, blocks)
    else:
        rates = block_rates(tensor_sums[:tensors, :2], member)
        new_params = apply_update_plain(rank, rates, outer_params, updates, owners, own_rows)
    return (new_params, deinterleave(new_momentum, blocks))


def solution(mesh):
    return jax.shard_map(
        shards,
        mesh=mesh,
        in_specs=(P("shard", None), P("rep", "shard", None), P("shard", "rep"), P("shard")),
        out_specs=(P("shard", None), P("shard", "rep")),
        check_vma=False,
    )
```
